32 devices in a mesh: src: 4 (over y, x), dst: 8 (over z, core).
Axes of the slice: x: 2, y: 2, z: 4, core: 2. Of those that a mesh axis runs over, the one named last changes fastest.
Arguments:
- edge_in: bfloat16 [32768, 512], P(('src', 'dst')), may hold values from -6 to 6
- atom_in: bfloat16 [2048, 256], P(('dst', 'src')), may hold values from -6 to 6
- targets: int32 [32768], P(('src', 'dst')), may hold values from 0 to 255
- reverse: int32 [32768], P(('src', 'dst')), may hold values from 0 to 127, as said below
- counts: int32 [4, 8, 8], P('src', 'dst'), may hold values from 2 to 128, as said below
- w_in: bfloat16 [256, 512], replicated, may hold values from -0.375 to 0.375
- gains: float32 [2, 512], replicated, may hold values from 0.1 to 1.9
- w_layers: bfloat16 [2, 512, 512], replicated, may hold values from -0.25 to 0.25
- w_rev: bfloat16 [512, 512], replicated, may hold values from -0.25 to 0.25
- w_down: bfloat16 [512, 256], replicated, may hold values from -0.25 to 0.25
- w_atom: bfloat16 [256, 256], replicated, may hold values from -0.375 to 0.375
Outputs:
- edge_out: bfloat16 [32768, 512], P(('src', 'dst'))
- atom_out: bfloat16 [2048, 256], P(('dst', 'src'))
The draws below stay inside these ranges and needn't reach their ends.
Inputs may be any that keep to these rules, and one draw needn't show every extreme that they name: In every block k of tile (i, j), reverse maps the used slots one to one onto the used slots of block j of tile (i, k), and the two maps are inverse to each other; in block j of tile (i, j) it pairs used slots and is its own inverse. Unused slots map onto unused slots. Every count is even, and counts[i, j, k] equals counts[i, k, j].
All inputs are finite; a program needn't handle non-finite values.
Results may differ from the reference program's by a relative error of at most 0.014.
Values may be sent and summed in bfloat16 or wider, within the bound.
No kernel may reach another device: no remote copies, remote signals or barrier semaphores. Data moves between devices by JAX's collectives and lax.ppermute only.
A program may use at most 128 MiB of HBM per device.

```python
import jax
import jax.numpy as jnp
from jax import lax

W = 512
A = 256
LAYERS = 2
RB = 128
EDGE_DEV = 1024
EDGES = 32768
ATOM_PART = 256
ATOMS = 2048
N_SRC = 4
N_DST = 8


def mirror_tables(key):
    base = jax.random.fold_in(key, 7)
    key_count, key_order = jax.random.split(base, 2)
    lowest = max(1, RB // 16)
    raw = jax.random.randint(key_count, (N_SRC, N_DST, N_DST), lowest, RB // 2 + 1) * 2
    rows_j = jnp.arange(N_DST)[:, None]
    cols_k = jnp.arange(N_DST)[None, :]
    count = jnp.where(rows_j <= cols_k, raw, jnp.transpose(raw, (0, 2, 1))).astype(jnp.int32)
    slot = jnp.arange(RB).astype(jnp.int32)
    noise = jax.random.randint(key_order, (N_SRC, N_DST, N_DST, RB), 0, 2 ** 14)
    scores = (slot >= count[..., None]).astype(jnp.int32) * 2 ** 24 + noise * RB + slot
    order = jnp.argsort(scores, axis=-1, stable=True).astype(jnp.int32)
    other = jnp.transpose(order, (0, 2, 1, 3))
    partner = order[..., jnp.bitwise_xor(slot, 1)]
    diagonal = (rows_j == cols_k)[None, :, :, None]
    value = jnp.where(diagonal, partner, other)
    inverse = jnp.argsort(order, axis=-1, stable=True).astype(jnp.int32)
    back = jnp.take_along_axis(value, inverse, axis=-1).astype(jnp.int32)
    return (back.reshape(N_SRC * N_DST * N_DST * RB), count)


def draw_reverse(key, part):
    return mirror_tables(key)[0]


def draw_counts(key, part):
    return mirror_tables(key)[1]


def touch_ends(values, own_key, least, high):
    longest = values.shape.index(max(values.shape))
    spots = []
    for shift in (0, 1):
        where = [jax.random.randint(jax.random.fold_in(own_key, axis), (), 0, length) for axis, length in enumerate(values.shape)]
        where[longest] = (where[longest] + shift) % values.shape[longest]
        spots.append(tuple(where))
    return values.at[spots[0]].set(least).at[spots[1]].set(high)


def block_scale(own_key, extent, cuts, smallest, top_value):
    level, own = 1.0, jax.random.fold_in(own_key, 6)
    for axis_at, parts in cuts:
        draws = jnp.exp(jax.random.uniform(jax.random.fold_in(own, axis_at), (parts,), jnp.float32, smallest / len(cuts), top_value / len(cuts)))
        level = level * jnp.repeat(draws, extent[axis_at] // parts).reshape([-1 if axis == axis_at else 1 for axis in range(len(extent))])
    return level


def scatter_about(rng, dims, scale, limit, pieces=(), held_as=jnp.bfloat16):
    factor_of = block_scale(rng, dims, pieces, -0.22, 0.18) if pieces else 1.0
    entries = jax.random.normal(rng, dims, jnp.float32) * scale * factor_of
    return jnp.minimum(jnp.maximum(entries, -limit), limit).astype(held_as)


def setup_inputs(seed: int = 0) -> dict:
    splits = jax.random.split(jax.random.key(seed), 12)
    return {
        "edge_in": scatter_about(splits[0], (EDGES, W), 1.0, 6.0, ((0, 32),)),
        "atom_in": scatter_about(splits[1], (ATOMS, A), 1.0, 6.0, ((0, 32),)),
        "targets": touch_ends(jax.random.randint(splits[2], (EDGES,), 0, ATOM_PART), jax.random.fold_in(splits[2], 1), 0, ATOM_PART - 1).astype(jnp.int32),
        "reverse": draw_reverse(jax.random.fold_in(splits[11], 71), 0),
        "counts": draw_counts(jax.random.fold_in(splits[11], 71), 0),
        "w_in": scatter_about(splits[5], (A, W), A ** -0.5, 0.375),
        "gains": jnp.clip(1.0 + 0.18 * jax.random.normal(splits[6], (LAYERS, W), jnp.float32), 0.1, 1.9),
        "w_layers": scatter_about(splits[7], (LAYERS, W, W), W ** -0.5, 0.25),
        "w_rev": scatter_about(splits[8], (W, W), W ** -0.5, 0.25),
        "w_down": scatter_about(splits[9], (W, A), W ** -0.5, 0.25),
        "w_atom": scatter_about(splits[10], (A, A), A ** -0.5, 0.375),
    }


def edge_layers(base, picked, gains, w_layers):
    state = base.astype(jnp.float32) + picked.astype(jnp.float32)
    for layer in range(LAYERS):
        scale = lax.rsqrt(lax.optimization_barrier(jnp.mean(state * state, axis=-1, keepdims=True)) + 1e-06)
        normed = (state * scale * gains[layer]).astype(jnp.bfloat16)
        state = state + jax.nn.silu(jnp.dot(normed, w_layers[layer], preferred_element_type=jnp.float32))
    return state

def reference(edge_in, atom_in, targets, reverse, counts, w_in, gains, w_layers, w_rev, w_down, w_atom):
    row_len = N_DST * EDGE_DEV
    atom_proj = jnp.dot(atom_in, w_in, preferred_element_type=jnp.float32).astype(jnp.bfloat16)
    place = jnp.arange(row_len).astype(jnp.int32)
    column = place // EDGE_DEV
    block = place % EDGE_DEV // RB
    slot = place % RB

    def one_row(total, item):
        edges, targ, back, count = item
        used = slot < count[column, block]
        atom_ids = (column * ATOM_PART + targ).astype(jnp.int32)
        picked = jnp.take(atom_proj, atom_ids, axis=0)
        state = edge_layers(edges, picked, gains, w_layers)
        sent = state.astype(jnp.bfloat16)
        source = (block * EDGE_DEV + column * RB + back).astype(jnp.int32)
        mirrored = jnp.take(sent, source, axis=0)
        combined = jnp.where(used[:, None], state + jnp.dot(mirrored, w_rev, preferred_element_type=jnp.float32), jnp.float32(0.0))
        result = combined.astype(jnp.bfloat16)
        contrib = jnp.where(used[:, None], jnp.dot(result, w_down, preferred_element_type=jnp.float32), jnp.float32(0.0))
        total = total + jax.ops.segment_sum(contrib, atom_ids, num_segments=ATOMS)
        return (total, result)
    items = (edge_in.reshape(N_SRC, row_len, W), targets.reshape(N_SRC, row_len), reverse.reshape(N_SRC, row_len), counts)
    agg, outs = lax.scan(one_row, jnp.zeros((ATOMS, A), jnp.float32), items)
    act = jax.nn.silu(0.3 * agg).astype(jnp.bfloat16)
    atom_out = (atom_in.astype(jnp.float32) + jnp.dot(act, w_atom, preferred_element_type=jnp.float32)).astype(jnp.bfloat16)
    return (outs.reshape(EDGES, W), atom_out)
```

```python
import functools

import jax
import jax.numpy as jnp
from jax import lax
from jax.experimental import pallas as pl
from jax.experimental.pallas import tpu as pltpu
from jax.sharding import PartitionSpec as P

F32 = jnp.float32
BF16 = jnp.bfloat16
LIMIT = 16 * 2**20


def dot(a, b):
    return jnp.dot(a, b, preferred_element_type=F32)


def column(row, width):
    n = row.shape[1]
    spread = jnp.transpose(jnp.broadcast_to(row, (n, n)))
    return jnp.concatenate([spread] * (width // n), axis=1)


def relabel(row, me, share):
    return (lax.div(row, share) ^ me) * share + lax.rem(row, share)


def layers(x, gains_ref, weights, first):
    feat = x.shape[1]
    for layer in range(gains_ref.shape[0]):
        scale = lax.rsqrt(jnp.mean(x * x, axis=-1, keepdims=True) + 1e-06)
        normed = (x * scale * gains_ref[layer : layer + 1, :]).astype(BF16)
        y = dot(normed, weights[first + layer * feat : first + (layer + 1) * feat])
        x = x + y / (1.0 + jnp.exp(-y))
    return x


def edge_kernel(ds, shards, meta, *refs):
    group = len(ds)
    edges = refs[:group]
    atoms = refs[group : group + shards]
    targets, reverse, gains, weights = refs[group + shards : group + shards + 4]
    x_ref, *msgs = refs[-1 - group :]
    width = edges[0].shape[0]
    share = atoms[0].shape[0]
    me = meta[0]
    hidden, feat = atoms[0].shape[1], edges[0].shape[1]
    w_rev = hidden + gains.shape[0] * feat
    table = jnp.concatenate([a[...] for a in atoms], axis=0)
    lanes = lax.broadcasted_iota(jnp.int32, (width, table.shape[0]), 1)
    picks = []
    for g in range(group):
        row = relabel(targets[pl.ds(meta[1] ^ ds[g], 1), :], me, share)
        picks.append((column(row, table.shape[0]) == lanes).astype(BF16))
    picked = dot(jnp.concatenate(picks, axis=0), table).astype(BF16)
    proj = dot(picked, weights[:hidden]).astype(BF16).astype(F32)
    x = jnp.concatenate([e[...] for e in edges], axis=0).astype(F32) + proj
    x = layers(x, gains, weights, hidden)
    sent = x.astype(BF16)
    rows = lax.broadcasted_iota(jnp.int32, (width, width), 0)
    slots = lax.broadcasted_iota(jnp.int32, (width, x.shape[1]), 0)
    turned = []
    for g in range(group):
        k = meta[1] ^ ds[g]
        used = meta[2 + k]
        mine = slice(g * width, (g + 1) * width)
        x_ref[mine, :] = jnp.where(slots < used, x[mine], 0.0)
        swap = (rows == reverse[pl.ds(k, 1), :]) & (rows < used)
        turned.append(dot(swap.astype(BF16), sent[mine]).astype(BF16))
    msg = dot(jnp.concatenate(turned, axis=0), weights[w_rev:]).astype(BF16)
    for g in range(group):
        msgs[g][...] = msg[g * width : (g + 1) * width]


def edge_group(ds, edge_in, atoms, targets, reverse, meta, gains, weights, after):
    _, width = targets.shape
    group = len(ds)
    feat = edge_in.shape[1]
    whole = pl.BlockSpec(memory_space=pltpu.VMEM)
    picks = [
        pl.BlockSpec((width, feat), functools.partial(lambda i, m, d: (m[1] ^ d, 0), d=d))
        for d in ds
    ]
    rows = group * width
    return pl.pallas_call(
        functools.partial(edge_kernel, ds, len(atoms)),
        out_shape=[jax.ShapeDtypeStruct((rows, feat), F32)]
        + [jax.ShapeDtypeStruct((width, feat), BF16)] * group,
        grid_spec=pltpu.PrefetchScalarGridSpec(
            num_scalar_prefetch=1,
            grid=(1,),
            in_specs=picks + [whole] * (len(atoms) + 4) + [pl.BlockSpec(memory_space=pl.ANY)] * len(after),
            out_specs=[whole] * (1 + group),
        ),
        cost_estimate=pl.CostEstimate(
            flops=2 * rows * feat * feat * 4, bytes_accessed=rows * feat * 8, transcendentals=rows * feat * 4
        ),
        compiler_params=pltpu.CompilerParams(vmem_limit_bytes=LIMIT),
        name="edge_group",
    )(meta, *[edge_in] * group, *atoms, targets, reverse, gains, weights, *after)


def finish_kernel(ds, first, last, shards, meta, *refs):
    group = len(ds)
    xs, msgs = refs[:group], refs[group : 2 * group]
    targets, w_down = refs[2 * group : 2 * group + 2]
    rest = list(refs[2 * group + 2 :])
    acc = None if first else rest[0]
    out, *sums = rest[0 if first else 2 : -2]
    stage, sems = rest[-2:]
    width = msgs[0].shape[0]
    copies = []
    for g, d in enumerate(ds):
        k = meta[1] ^ d
        x = xs[g][...] + msgs[g][...].astype(F32)
        stage[pl.ds(g * width, width), :] = x.astype(BF16)
        copies.append(
            pltpu.make_async_copy(
                stage.at[pl.ds(g * width, width), :],
                out.at[pl.ds(pl.multiple_of(k * width, width), width), :],
                sems.at[g],
            )
        )
        copies[g].start()
    contrib = dot(stage[...], w_down[...]).astype(BF16)
    atoms = sums[0].shape[0] * (shards if last else 1)
    place = lax.broadcasted_iota(jnp.int32, (atoms, width), 0)
    spread = [
        (place == relabel(targets[pl.ds(meta[1] ^ d, 1), :], meta[0], atoms // shards)).astype(BF16)
        for d in ds
    ]
    total = dot(jnp.concatenate(spread, axis=1), contrib)
    if not first:
        total = total + acc[...]
    if last:
        share = atoms // shards
        for p in range(shards):
            sums[p][...] = total[p * share : (p + 1) * share].astype(sums[p].dtype)
    else:
        sums[0][...] = total
    for copy in copies:
        copy.wait()


def finish(ds, xs, msgs, targets, meta, w_down, acc, out, total_rows, atoms, shards, last):
    _, width = targets.shape
    feat, hidden = w_down.shape
    first = acc is None
    group = len(ds)
    whole = pl.BlockSpec(memory_space=pltpu.VMEM)
    far = pl.BlockSpec(memory_space=pl.ANY)
    share = atoms // shards
    if last:
        tail = [jax.ShapeDtypeStruct((share, hidden), F32)]
        tail += [jax.ShapeDtypeStruct((share, hidden), BF16)] * (shards - 1)
    else:
        tail = [jax.ShapeDtypeStruct((atoms, hidden), F32)]
    return pl.pallas_call(
        functools.partial(finish_kernel, ds, first, last, shards),
        out_shape=[jax.ShapeDtypeStruct((total_rows, feat), BF16)] + tail,
        grid_spec=pltpu.PrefetchScalarGridSpec(
            num_scalar_prefetch=1,
            grid=(1,),
            in_specs=[
                pl.BlockSpec((width, feat), functools.partial(lambda i, m, at: (at, 0), at=at))
                for _, at in xs
            ]
            + [whole] * (group + 2)
            + ([] if first else [whole, far]),
            out_specs=[far] + [whole] * len(tail),
            scratch_shapes=[
                pltpu.VMEM((group * width, feat), BF16),
                pltpu.SemaphoreType.DMA((group,)),
            ],
        ),
        input_output_aliases={} if first else {2 * group + 4: 0},
        cost_estimate=pl.CostEstimate(
            flops=4 * group * width * feat * hidden,
            bytes_accessed=group * width * feat * 8,
            transcendentals=0,
        ),
        compiler_params=pltpu.CompilerParams(vmem_limit_bytes=LIMIT),
        name="finish",
    )(meta, *[x for x, _ in xs], *msgs, targets, w_down, *([] if first else [acc, out]))


def atom_kernel(atom_in, w_atom, *refs):
    *parts, out = refs
    agg = parts[0][...]
    for part in parts[1:]:
        agg = agg + part[...].astype(F32)
    v = 0.3 * agg
    act = (v / (1.0 + jnp.exp(-v))).astype(BF16)
    out[...] = (atom_in[...].astype(F32) + dot(act, w_atom[...])).astype(BF16)


def edge_order(blocks):
    half = blocks // 2
    near = [[d, d + 1] for d in range(2, half, 2)]
    far = [[d, d + 1] for d in range(half + 2, blocks, 2)]
    return [[half], [half + 1]] + near + far + [[1, 0]]


def on_device(
    edge_in, atom_in, targets, reverse, counts, w_in, gains, w_layers, w_rev, w_down, w_atom
):
    slots, feat = edge_in.shape
    blocks = counts.shape[2]
    width = slots // blocks
    shards = lax.axis_size("src")
    atoms = atom_in.shape[0] * shards
    me, part = lax.axis_index("src"), lax.axis_index("dst")
    meta = jnp.concatenate([jnp.stack([me, part]).astype(jnp.int32), counts.reshape(blocks)])
    targets = targets.reshape(blocks, width)
    reverse = reverse.reshape(blocks, width)

    def over(size, d):
        return [(s, s ^ d) for s in range(size)]

    held = [atom_in]
    for p in range(1, shards):
        held.append(lax.ppermute(atom_in, "src", over(shards, p)))
    weights = jnp.concatenate([w_in, w_layers.reshape(-1, feat), w_rev], axis=0)
    xs, msgs, after = {}, {}, []
    for ds in edge_order(blocks):
        x, *sent = edge_group(ds, edge_in, held, targets, reverse, meta, gains, weights, after)
        after = [x]
        for g, d in enumerate(ds):
            xs[d] = (x, g)
            msgs[d] = sent[g]
            if d:
                msgs[d] = lax.ppermute(sent[g], "dst", over(blocks, d))
    acc = out = None
    half = blocks // 2
    for at in [0, half] + list(range(2, half, 2)) + list(range(half + 2, blocks, 2)):
        ds = [at, at + 1]
        last = at + 2 == blocks
        out, *sums = finish(
            ds, [xs[d] for d in ds], [msgs[d] for d in ds], targets, meta,
            w_down, acc, out, slots, atoms, shards, last,
        )
        acc = sums[0]
    parts = [sums[0]]
    for p in range(1, shards):
        parts.append(lax.ppermute(sums[p], "src", over(shards, p)))
    atom_out = pl.pallas_call(
        atom_kernel,
        out_shape=jax.ShapeDtypeStruct(atom_in.shape, BF16),
        compiler_params=pltpu.CompilerParams(vmem_limit_bytes=LIMIT),
        name="atom_update",
    )(atom_in, w_atom, *parts)
    return (out, atom_out)


def solution(mesh):
    placed = (
        P(("src", "dst"), None),
        P(("dst", "src"), None),
        P(("src", "dst")),
        P(("src", "dst")),
        P("src", "dst", None),
        P(),
        P(),
        P(),
        P(),
        P(),
        P(),
    )
    return jax.shard_map(
        on_device,
        mesh=mesh,
        in_specs=placed,
        out_specs=(P(("src", "dst"), None), P(("dst", "src"), None)),
        check_vma=False,
    )
```

```python
import functools

import jax
import jax.numpy as jnp
from jax import lax
from jax.experimental import pallas as pl
from jax.experimental.pallas import tpu as pltpu
from jax.sharding import PartitionSpec as P

F32 = jnp.float32
BF16 = jnp.bfloat16
LIMIT = 16 * 2**20


def dot(a, b):
    return jnp.dot(a, b, preferred_element_type=F32)


def column(row, width):
    n = row.shape[1]
    spread = jnp.transpose(jnp.broadcast_to(row, (n, n)))
    return jnp.concatenate([spread] * (width // n), axis=1)


def relabel(row, me, share):
    return (lax.div(row, share) ^ me) * share + lax.rem(row, share)


def layers(x, gains_ref, weights, first):
    feat = x.shape[1]
    for layer in range(gains_ref.shape[0]):
        scale = lax.rsqrt(jnp.mean(x * x, axis=-1, keepdims=True) + 1e-06)
        normed = (x * scale * gains_ref[layer : layer + 1, :]).astype(BF16)
        y = dot(normed, weights[first + layer * feat : first + (layer + 1) * feat])
        x = x + y / (1.0 + jnp.exp(-y))
    return x


def edge_kernel(ds, shards, meta, *refs):
    group = len(ds)
    edge_in, *atoms = refs[: 1 + shards]
    targets, reverse, gains, weights = refs[1 + shards : 5 + shards]
    x_ref, *msgs = refs[-1 - group :]
    width = targets.shape[1]
    share = atoms[0].shape[0]
    me = meta[0]
    hidden, feat = atoms[0].shape[1], edge_in.shape[1]
    w_rev = hidden + gains.shape[0] * feat
    table = jnp.concatenate([a[...] for a in atoms], axis=0)
    lanes = lax.broadcasted_iota(jnp.int32, (width, table.shape[0]), 1)
    picks = []
    for g in range(group):
        row = relabel(targets[pl.ds(meta[1] ^ ds[g], 1), :], me, share)
        picks.append((column(row, table.shape[0]) == lanes).astype(BF16))
    picked = dot(jnp.concatenate(picks, axis=0), table).astype(BF16)
    proj = dot(picked, weights[:hidden]).astype(BF16).astype(F32)
    starts = [pl.multiple_of((meta[1] ^ d) * width, width) for d in ds]
    x = jnp.concatenate([edge_in[pl.ds(start, width), :] for start in starts], axis=0)
    x = x.astype(F32) + proj
    x = layers(x, gains, weights, hidden)
    sent = x.astype(BF16)
    rows = lax.broadcasted_iota(jnp.int32, (width, width), 0)
    slots = lax.broadcasted_iota(jnp.int32, (width, x.shape[1]), 0)
    turned = []
    for g in range(group):
        k = meta[1] ^ ds[g]
        used = meta[2 + k]
        mine = slice(g * width, (g + 1) * width)
        x_ref[mine, :] = jnp.where(slots < used, x[mine], 0.0)
        swap = (rows == reverse[pl.ds(k, 1), :]) & (rows < used)
        turned.append(dot(swap.astype(BF16), sent[mine]).astype(BF16))
    msg = dot(jnp.concatenate(turned, axis=0), weights[w_rev:]).astype(BF16)
    for g in range(group):
        msgs[g][...] = msg[g * width : (g + 1) * width]


def edge_group(ds, edge_in, atoms, targets, reverse, meta, gains, weights, after):
    _, width = targets.shape
    group = len(ds)
    feat = edge_in.shape[1]
    whole = pl.BlockSpec(memory_space=pltpu.VMEM)
    rows = group * width
    return pl.pallas_call(
        functools.partial(edge_kernel, ds, len(atoms)),
        out_shape=[jax.ShapeDtypeStruct((rows, feat), F32)]
        + [jax.ShapeDtypeStruct((width, feat), BF16)] * group,
        grid_spec=pltpu.PrefetchScalarGridSpec(
            num_scalar_prefetch=1,
            grid=(1,),
            in_specs=[whole] * (len(atoms) + 5) + [pl.BlockSpec(memory_space=pl.ANY)] * len(after),
            out_specs=[whole] * (1 + group),
        ),
        cost_estimate=pl.CostEstimate(
            flops=2 * rows * feat * feat * 4, bytes_accessed=rows * feat * 8, transcendentals=rows * feat * 4
        ),
        compiler_params=pltpu.CompilerParams(vmem_limit_bytes=LIMIT),
        name="edge_group",
    )(meta, edge_in, *atoms, targets, reverse, gains, weights, *after)


def finish_kernel(ds, ats, first, last, shards, meta, *refs):
    group = len(ds)
    xs, msgs = refs[:group], refs[group : 2 * group]
    targets, w_down = refs[2 * group : 2 * group + 2]
    rest = list(refs[2 * group + 2 :])
    acc = None if first else rest[0]
    out, *sums = rest[0 if first else 2 : -2]
    stage, sems = rest[-2:]
    width = msgs[0].shape[0]
    copies = []
    for g, d in enumerate(ds):
        k = meta[1] ^ d
        x = xs[g][pl.ds(ats[g] * width, width), :] + msgs[g][...].astype(F32)
        stage[pl.ds(g * width, width), :] = x.astype(BF16)
        copies.append(
            pltpu.make_async_copy(
                stage.at[pl.ds(g * width, width), :],
                out.at[pl.ds(pl.multiple_of(k * width, width), width), :],
                sems.at[g],
            )
        )
        copies[g].start()
    contrib = dot(stage[...], w_down[...]).astype(BF16)
    atoms = sums[0].shape[0] * (shards if last else 1)
    place = lax.broadcasted_iota(jnp.int32, (atoms, width), 0)
    spread = [
        (place == relabel(targets[pl.ds(meta[1] ^ d, 1), :], meta[0], atoms // shards)).astype(BF16)
        for d in ds
    ]
    total = dot(jnp.concatenate(spread, axis=1), contrib)
    if not first:
        total = total + acc[...]
    if last:
        share = atoms // shards
        for p in range(shards):
            sums[p][...] = total[p * share : (p + 1) * share].astype(sums[p].dtype)
    else:
        sums[0][...] = total
    for copy in copies:
        copy.wait()


def finish(ds, xs, msgs, targets, meta, w_down, acc, out, total_rows, atoms, shards, last):
    _, width = targets.shape
    feat, hidden = w_down.shape
    first = acc is None
    group = len(ds)
    whole = pl.BlockSpec(memory_space=pltpu.VMEM)
    far = pl.BlockSpec(memory_space=pl.ANY)
    share = atoms // shards
    if last:
        tail = [jax.ShapeDtypeStruct((share, hidden), F32)]
        tail += [jax.ShapeDtypeStruct((share, hidden), BF16)] * (shards - 1)
    else:
        tail = [jax.ShapeDtypeStruct((atoms, hidden), F32)]
    return pl.pallas_call(
        functools.partial(finish_kernel, ds, [at for _, at in xs], first, last, shards),
        out_shape=[jax.ShapeDtypeStruct((total_rows, feat), BF16)] + tail,
        grid_spec=pltpu.PrefetchScalarGridSpec(
            num_scalar_prefetch=1,
            grid=(1,),
            in_specs=[whole] * (2 * group + 2)
            + ([] if first else [whole, far]),
            out_specs=[far] + [whole] * len(tail),
            scratch_shapes=[
                pltpu.VMEM((group * width, feat), BF16),
                pltpu.SemaphoreType.DMA((group,)),
            ],
        ),
        input_output_aliases={} if first else {2 * group + 4: 0},
        cost_estimate=pl.CostEstimate(
            flops=4 * group * width * feat * hidden,
            bytes_accessed=group * width * feat * 8,
            transcendentals=0,
        ),
        compiler_params=pltpu.CompilerParams(vmem_limit_bytes=LIMIT),
        name="finish",
    )(meta, *[x for x, _ in xs], *msgs, targets, w_down, *([] if first else [acc, out]))


def atom_kernel(atom_in, w_atom, *refs):
    *parts, out = refs
    agg = parts[0][...]
    for part in parts[1:]:
        agg = agg + part[...].astype(F32)
    v = 0.3 * agg
    act = (v / (1.0 + jnp.exp(-v))).astype(BF16)
    out[...] = (atom_in[...].astype(F32) + dot(act, w_atom[...])).astype(BF16)


def edge_order(blocks):
    half = blocks // 2
    near = [[d, d + 1] for d in range(2, half, 2)]
    far = [[d, d + 1] for d in range(half + 2, blocks, 2)]
    return [[half, half + 1]] + near + far + [[1, 0]]


def on_device(
    edge_in, atom_in, targets, reverse, counts, w_in, gains, w_layers, w_rev, w_down, w_atom
):
    slots, feat = edge_in.shape
    blocks = counts.shape[2]
    width = slots // blocks
    shards = lax.axis_size("src")
    atoms = atom_in.shape[0] * shards
    me, part = lax.axis_index("src"), lax.axis_index("dst")
    meta = jnp.concatenate([jnp.stack([me, part]).astype(jnp.int32), counts.reshape(blocks)])
    targets = targets.reshape(blocks, width)
    reverse = reverse.reshape(blocks, width)

    def over(size, d):
        return [(s, s ^ d) for s in range(size)]

    held = [atom_in]
    for p in range(1, shards):
        held.append(lax.ppermute(atom_in, "src", over(shards, p)))
    weights = jnp.concatenate([w_in, w_layers.reshape(-1, feat), w_rev], axis=0)
    xs, msgs, after = {}, {}, []
    for ds in edge_order(blocks):
        x, *sent = edge_group(ds, edge_in, held, targets, reverse, meta, gains, weights, after)
        after = [x]
        for g, d in enumerate(ds):
            xs[d] = (x, g)
            msgs[d] = sent[g]
            if d:
                msgs[d] = lax.ppermute(sent[g], "dst", over(blocks, d))
    acc = out = None
    half = blocks // 2
    groups = [[0, 1, half, half + 1]]
    rest = list(range(2, half)) + list(range(half + 2, blocks))
    groups += [rest[n : n + 4] for n in range(0, len(rest), 4)]
    for ds in groups:
        last = ds is groups[-1]
        out, *sums = finish(
            ds, [xs[d] for d in ds], [msgs[d] for d in ds], targets, meta,
            w_down, acc, out, slots, atoms, shards, last,
        )
        acc = sums[0]
    parts = [sums[0]]
    for p in range(1, shards):
        parts.append(lax.ppermute(sums[p], "src", over(shards, p)))
    atom_out = pl.pallas_call(
        atom_kernel,
        out_shape=jax.ShapeDtypeStruct(atom_in.shape, BF16),
        compiler_params=pltpu.CompilerParams(vmem_limit_bytes=LIMIT),
        name="atom_update",
    )(atom_in, w_atom, *parts)
    return (out, atom_out)


def solution(mesh):
    placed = (
        P(("src", "dst"), None),
        P(("dst", "src"), None),
        P(("src", "dst")),
        P(("src", "dst")),
        P("src", "dst", None),
        P(),
        P(),
        P(),
        P(),
        P(),
        P(),
    )
    return jax.shard_map(
        on_device,
        mesh=mesh,
        in_specs=placed,
        out_specs=(P(("src", "dst"), None), P(("dst", "src"), None)),
        check_vma=False,
    )
```

```python
import functools

import jax
import jax.numpy as jnp
from jax import lax
from jax.experimental import pallas as pl
from jax.experimental.pallas import tpu as pltpu
from jax.sharding import PartitionSpec as P

F32 = jnp.float32
BF16 = jnp.bfloat16
LIMIT = 16 * 2**20


def dot(a, b):
    return jnp.dot(a, b, preferred_element_type=F32)


def column(row, width):
    n = row.shape[1]
    spread = jnp.transpose(jnp.broadcast_to(row, (n, n)))
    return jnp.concatenate([spread] * (width // n), axis=1)


def relabel(row, me, share):
    return (lax.div(row, share) ^ me) * share + lax.rem(row, share)


def silu(v):
    half = 0.5 * v
    return half + half * jnp.tanh(half)


def layers(x, gains_ref, weights, first):
    feat = x.shape[1]
    for layer in range(gains_ref.shape[0]):
        scale = lax.rsqrt(jnp.mean(x * x, axis=-1, keepdims=True) + 1e-06)
        normed = (x * scale * gains_ref[layer : layer + 1, :]).astype(BF16)
        y = dot(normed, weights[first + layer * feat : first + (layer + 1) * feat])
        x = x + silu(y)
    return x


def edge_kernel(ds, shards, *refs):
    group = len(ds)
    me, part = lax.axis_index("src"), lax.axis_index("dst")
    edge_in, *atoms = refs[: 1 + shards]
    targets, reverse, counts, gains, weights = refs[1 + shards : 6 + shards]
    x_ref, *msgs = refs[-1 - group :]
    width = targets.shape[1]
    share = atoms[0].shape[0]
    hidden, feat = atoms[0].shape[1], edge_in.shape[1]
    w_rev = hidden + gains.shape[0] * feat
    table = jnp.concatenate([a[...] for a in atoms], axis=0)
    lanes = lax.broadcasted_iota(jnp.int32, (width, table.shape[0]), 1)
    picks = []
    for g in range(group):
        row = relabel(targets[pl.ds(part ^ ds[g], 1), :], me, share)
        picks.append((column(row, table.shape[0]) == lanes).astype(BF16))
    picked = dot(jnp.concatenate(picks, axis=0), table).astype(BF16)
    proj = dot(picked, weights[:hidden]).astype(BF16).astype(F32)
    starts = [pl.multiple_of((part ^ d) * width, width) for d in ds]
    x = jnp.concatenate([edge_in[pl.ds(start, width), :] for start in starts], axis=0)
    x = x.astype(F32) + proj
    x = layers(x, gains, weights, hidden)
    sent = x.astype(BF16)
    rows = lax.broadcasted_iota(jnp.int32, (width, width), 0)
    slots = lax.broadcasted_iota(jnp.int32, (width, x.shape[1]), 0)
    turned = []
    for g in range(group):
        k = part ^ ds[g]
        lanes = lax.broadcasted_iota(jnp.int32, counts.shape, 1)
        used = jnp.sum(jnp.where(lanes == k, counts[...], 0), axis=1, keepdims=True)
        mine = slice(g * width, (g + 1) * width)
        x_ref[mine, :] = jnp.where(slots < used, x[mine], 0.0)
        swap = (rows == reverse[pl.ds(k, 1), :]) & (rows < used)
        turned.append(dot(swap.astype(BF16), sent[mine]).astype(BF16))
    msg = dot(jnp.concatenate(turned, axis=0), weights[w_rev:]).astype(BF16)
    for g in range(group):
        msgs[g][...] = msg[g * width : (g + 1) * width]


def edge_group(ds, edge_in, atoms, targets, reverse, counts, gains, weights, after):
    _, width = targets.shape
    group = len(ds)
    feat = edge_in.shape[1]
    whole = pl.BlockSpec(memory_space=pltpu.VMEM)
    rows = group * width
    return pl.pallas_call(
        functools.partial(edge_kernel, ds, len(atoms)),
        out_shape=[jax.ShapeDtypeStruct((rows, feat), F32)]
        + [jax.ShapeDtypeStruct((width, feat), BF16)] * group,
        in_specs=[whole] * (len(atoms) + 6) + [pl.BlockSpec(memory_space=pl.ANY)] * len(after),
        out_specs=[whole] * (1 + group),
        cost_estimate=pl.CostEstimate(
            flops=2 * rows * feat * feat * 4, bytes_accessed=rows * feat * 8, transcendentals=rows * feat * 4
        ),
        compiler_params=pltpu.CompilerParams(vmem_limit_bytes=LIMIT),
        name="edge_group",
    )(edge_in, *atoms, targets, reverse, counts, gains, weights, *after)


def block_copy(stage, g, out, k, width, sems):
    return pltpu.make_async_copy(
        stage.at[pl.ds(g * width, width), :],
        out.at[pl.ds(pl.multiple_of(k * width, width), width), :],
        sems.at[g],
    )


def store_kernel(ds, width, stage, old, out, sems):
    part = lax.axis_index("dst")
    copies = [block_copy(stage, g, out, part ^ d, width, sems) for g, d in enumerate(ds)]
    for copy in copies:
        copy.start()
    for copy in copies:
        copy.wait()


def store(ds, width, stage, out):
    far = pl.BlockSpec(memory_space=pl.ANY)
    return pl.pallas_call(
        functools.partial(store_kernel, ds, width),
        out_shape=jax.ShapeDtypeStruct(out.shape, out.dtype),
        in_specs=[pl.BlockSpec(memory_space=pltpu.VMEM), far],
        out_specs=far,
        scratch_shapes=[pltpu.SemaphoreType.DMA((len(ds),))],
        input_output_aliases={1: 0},
        cost_estimate=pl.CostEstimate(flops=10**8, bytes_accessed=stage.size * 4, transcendentals=0),
        compiler_params=pltpu.CompilerParams(vmem_limit_bytes=LIMIT),
        name="store",
    )(stage, out)


def finish_kernel(ds, ats, first, last, shards, *refs):
    group = len(ds)
    me, part = lax.axis_index("src"), lax.axis_index("dst")
    xs, msgs = refs[:group], refs[group : 2 * group]
    targets, w_down = refs[2 * group : 2 * group + 2]
    rest = list(refs[2 * group + 2 :])
    acc = None if first else rest[0]
    if last:
        stage, *sums = rest[1:]
    else:
        out, *sums = rest[0 if first else 2 : -2]
        stage, sems = rest[-2:]
    width = msgs[0].shape[0]
    copies = []
    for g, d in enumerate(ds):
        x = xs[g][pl.ds(ats[g] * width, width), :] + msgs[g][...].astype(F32)
        stage[pl.ds(g * width, width), :] = x.astype(BF16)
        if not last:
            copies.append(block_copy(stage, g, out, part ^ d, width, sems))
            copies[g].start()
    contrib = dot(stage[...], w_down[...]).astype(BF16)
    atoms = sums[0].shape[0] * (shards if last else 1)
    place = lax.broadcasted_iota(jnp.int32, (atoms, width), 0)
    spread = [
        (place == relabel(targets[pl.ds(part ^ d, 1), :], me, atoms // shards)).astype(BF16)
        for d in ds
    ]
    total = dot(jnp.concatenate(spread, axis=1), contrib)
    if not first:
        total = total + acc[...]
    if last:
        share = atoms // shards
        for p in range(shards):
            sums[p][...] = total[p * share : (p + 1) * share].astype(sums[p].dtype)
    else:
        sums[0][...] = total
    for copy in copies:
        copy.wait()


def finish(ds, xs, msgs, targets, w_down, acc, out, total_rows, atoms, shards, last):
    _, width = targets.shape
    feat, hidden = w_down.shape
    first = acc is None
    assert not (first and last)
    group = len(ds)
    whole = pl.BlockSpec(memory_space=pltpu.VMEM)
    far = pl.BlockSpec(memory_space=pl.ANY)
    share = atoms // shards
    if last:
        tail = [jax.ShapeDtypeStruct((share, hidden), F32)]
        tail += [jax.ShapeDtypeStruct((share, hidden), BF16)] * (shards - 1)
    else:
        tail = [jax.ShapeDtypeStruct((atoms, hidden), F32)]
    return pl.pallas_call(
        functools.partial(finish_kernel, ds, [at for _, at in xs], first, last, shards),
        out_shape=[jax.ShapeDtypeStruct((group * width if last else total_rows, feat), BF16)] + tail,
        in_specs=[whole] * (2 * group + 2) + ([] if first else [whole] if last else [whole, far]),
        out_specs=[whole if last else far] + [whole] * len(tail),
        scratch_shapes=[]
        if last
        else [
            pltpu.VMEM((group * width, feat), BF16),
            pltpu.SemaphoreType.DMA((group,)),
        ],
        input_output_aliases={} if first or last else {2 * group + 3: 0},
        cost_estimate=pl.CostEstimate(
            flops=4 * group * width * feat * hidden,
            bytes_accessed=group * width * feat * 8,
            transcendentals=0,
        ),
        compiler_params=pltpu.CompilerParams(vmem_limit_bytes=LIMIT),
        name="finish",
    )(*[x for x, _ in xs], *msgs, targets, w_down, *([] if first else [acc] if last else [acc, out]))


def atom_kernel(atom_in, w_atom, *refs):
    *parts, out = refs
    agg = parts[0][...]
    for part in parts[1:]:
        agg = agg + part[...].astype(F32)
    v = 0.3 * agg
    act = silu(v).astype(BF16)
    out[...] = (atom_in[...].astype(F32) + dot(act, w_atom[...])).astype(BF16)


def edge_order(blocks):
    half = blocks // 2
    near = [[d, d + 1] for d in range(2, half, 2)]
    far = [[d, d + 1] for d in range(half + 2, blocks, 2)]
    return [[half, half + 1]] + near + far + [[1, 0]]


def on_device(
    edge_in, atom_in, targets, reverse, counts, w_in, gains, w_layers, w_rev, w_down, w_atom
):
    slots, feat = edge_in.shape
    blocks = counts.shape[2]
    width = slots // blocks
    shards = lax.axis_size("src")
    atoms = atom_in.shape[0] * shards
    counts = counts.reshape(1, blocks)
    targets = targets.reshape(blocks, width)
    reverse = reverse.reshape(blocks, width)

    def over(size, d):
        return [(s, s ^ d) for s in range(size)]

    held = [atom_in]
    for p in range(1, shards):
        held.append(lax.ppermute(atom_in, "src", over(shards, p)))
    weights = jnp.concatenate([w_in, w_layers.reshape(-1, feat), w_rev], axis=0)
    xs, msgs, after = {}, {}, []
    for ds in edge_order(blocks):
        x, *sent = edge_group(ds, edge_in, held, targets, reverse, counts, gains, weights, after)
        after = [x]
        for g, d in enumerate(ds):
            xs[d] = (x, g)
            msgs[d] = sent[g]
            if d:
                msgs[d] = lax.ppermute(sent[g], "dst", over(blocks, d))
    acc = out = None
    half = blocks // 2
    groups = [[0, 1, half, half + 1]]
    rest = list(range(2, half)) + list(range(half + 2, blocks))
    groups += [rest[n : n + 4] for n in range(0, len(rest), 4)]
    for ds in groups:
        last = ds is groups[-1]
        rows, *sums = finish(
            ds, [xs[d] for d in ds], [msgs[d] for d in ds], targets,
            w_down, acc, out, slots, atoms, shards, last,
        )
        acc = sums[0]
        if not last:
            out = rows
    parts = [sums[0]]
    for p in range(1, shards):
        parts.append(lax.ppermute(sums[p], "src", over(shards, p)))
    out = store(groups[-1], width, rows, out)
    atom_out = pl.pallas_call(
        atom_kernel,
        out_shape=jax.ShapeDtypeStruct(atom_in.shape, BF16),
        compiler_params=pltpu.CompilerParams(vmem_limit_bytes=LIMIT),
        name="atom_update",
    )(atom_in, w_atom, *parts)
    return (out, atom_out)


def solution(mesh):
    placed = (
        P(("src", "dst"), None),
        P(("dst", "src"), None),
        P(("src", "dst")),
        P(("src", "dst")),
        P("src", "dst", None),
        P(),
        P(),
        P(),
        P(),
        P(),
        P(),
    )
    return jax.shard_map(
        on_device,
        mesh=mesh,
        in_specs=placed,
        out_specs=(P(("src", "dst"), None), P(("dst", "src"), None)),
        check_vma=False,
    )
```

```python
import functools

import jax
import jax.numpy as jnp
from jax import lax
from jax.experimental import pallas as pl
from jax.experimental.pallas import tpu as pltpu
from jax.sharding import PartitionSpec as P

F32 = jnp.float32
BF16 = jnp.bfloat16
LIMIT = 16 * 2**20


def dot(a, b):
    return jnp.dot(a, b, preferred_element_type=F32)


def column(row, width):
    n = row.shape[1]
    spread = jnp.transpose(jnp.broadcast_to(row, (n, n)))
    return jnp.concatenate([spread] * (width // n), axis=1)


def relabel(row, me, share):
    return (lax.div(row, share) ^ me) * share + lax.rem(row, share)


def silu(v):
    half = 0.5 * v
    return half + half * jnp.tanh(half)


def layers(x, gains_ref, weights, first):
    feat = x.shape[1]
    for layer in range(gains_ref.shape[0]):
        scale = lax.rsqrt(jnp.mean(x * x, axis=-1, keepdims=True) + 1e-06)
        scaled = (x * gains_ref[layer : layer + 1, :]).astype(BF16)
        y = scale * dot(scaled, weights[first + layer * feat : first + (layer + 1) * feat])
        x = x + silu(y)
    return x


def edge_kernel(ds, shards, *refs):
    group = len(ds)
    me, part = lax.axis_index("src"), lax.axis_index("dst")
    edge_in, *atoms = refs[: 1 + shards]
    targets, reverse, counts, gains, weights = refs[1 + shards : 6 + shards]
    x_ref, *msgs = refs[-1 - group :]
    width = targets.shape[1]
    share = atoms[0].shape[0]
    hidden, feat = atoms[0].shape[1], edge_in.shape[1]
    w_rev = hidden + gains.shape[0] * feat
    table = jnp.concatenate([a[...] for a in atoms], axis=0)
    lanes = lax.broadcasted_iota(jnp.int32, (width, table.shape[0]), 1)
    picks = []
    for g in range(group):
        row = relabel(targets[pl.ds(part ^ ds[g], 1), :], me, share)
        picks.append((column(row, table.shape[0]) == lanes).astype(BF16))
    picked = dot(jnp.concatenate(picks, axis=0), table).astype(BF16)
    proj = dot(picked, weights[:hidden]).astype(BF16).astype(F32)
    starts = [pl.multiple_of((part ^ d) * width, width) for d in ds]
    x = jnp.concatenate([edge_in[pl.ds(start, width), :] for start in starts], axis=0)
    x = x.astype(F32) + proj
    x = layers(x, gains, weights, hidden)
    sent = x.astype(BF16)
    rows = lax.broadcasted_iota(jnp.int32, (width, width), 0)
    slots = lax.broadcasted_iota(jnp.int32, (width, x.shape[1]), 0)
    turned = []
    for g in range(group):
        k = part ^ ds[g]
        lanes = lax.broadcasted_iota(jnp.int32, counts.shape, 1)
        used = jnp.sum(jnp.where(lanes == k, counts[...], 0), axis=1, keepdims=True)
        mine = slice(g * width, (g + 1) * width)
        x_ref[mine, :] = jnp.where(slots < used, x[mine], 0.0)
        swap = (rows == reverse[pl.ds(k, 1), :]) & (rows < used)
        turned.append(dot(swap.astype(BF16), sent[mine]).astype(BF16))
    msg = dot(jnp.concatenate(turned, axis=0), weights[w_rev:]).astype(BF16)
    for g in range(group):
        msgs[g][...] = msg[g * width : (g + 1) * width]


def edge_group(ds, edge_in, atoms, targets, reverse, counts, gains, weights, after):
    _, width = targets.shape
    group = len(ds)
    feat = edge_in.shape[1]
    whole = pl.BlockSpec(memory_space=pltpu.VMEM)
    rows = group * width
    return pl.pallas_call(
        functools.partial(edge_kernel, ds, len(atoms)),
        out_shape=[jax.ShapeDtypeStruct((rows, feat), F32)]
        + [jax.ShapeDtypeStruct((width, feat), BF16)] * group,
        in_specs=[whole] * (len(atoms) + 6) + [pl.BlockSpec(memory_space=pl.ANY)] * len(after),
        out_specs=[whole] * (1 + group),
        cost_estimate=pl.CostEstimate(
            flops=2 * rows * feat * feat * 4, bytes_accessed=rows * feat * 8, transcendentals=rows * feat * 4
        ),
        compiler_params=pltpu.CompilerParams(vmem_limit_bytes=LIMIT),
        name="edge_group",
    )(edge_in, *atoms, targets, reverse, counts, gains, weights, *after)


def block_copy(stage, g, out, k, width, sems):
    return pltpu.make_async_copy(
        stage.at[pl.ds(g * width, width), :],
        out.at[pl.ds(pl.multiple_of(k * width, width), width), :],
        sems.at[g],
    )


def store_kernel(ds, width, stage, old, out, sems):
    part = lax.axis_index("dst")
    copies = [block_copy(stage, g, out, part ^ d, width, sems) for g, d in enumerate(ds)]
    for copy in copies:
        copy.start()
    for copy in copies:
        copy.wait()


def store(ds, width, stage, out):
    far = pl.BlockSpec(memory_space=pl.ANY)
    return pl.pallas_call(
        functools.partial(store_kernel, ds, width),
        out_shape=jax.ShapeDtypeStruct(out.shape, out.dtype),
        in_specs=[pl.BlockSpec(memory_space=pltpu.VMEM), far],
        out_specs=far,
        scratch_shapes=[pltpu.SemaphoreType.DMA((len(ds),))],
        input_output_aliases={1: 0},
        cost_estimate=pl.CostEstimate(flops=10**8, bytes_accessed=stage.size * 4, transcendentals=0),
        compiler_params=pltpu.CompilerParams(vmem_limit_bytes=LIMIT),
        name="store",
    )(stage, out)


def finish_kernel(ds, ats, first, last, shards, *refs):
    group = len(ds)
    me, part = lax.axis_index("src"), lax.axis_index("dst")
    xs, msgs = refs[:group], refs[group : 2 * group]
    targets, w_down = refs[2 * group : 2 * group + 2]
    rest = list(refs[2 * group + 2 :])
    acc = None if first else rest[0]
    if last:
        stage, *sums = rest[1:]
    else:
        out, *sums = rest[0 if first else 2 : -2]
        stage, sems = rest[-2:]
    width = msgs[0].shape[0]
    copies = []
    for g, d in enumerate(ds):
        x = xs[g][pl.ds(ats[g] * width, width), :] + msgs[g][...].astype(F32)
        stage[pl.ds(g * width, width), :] = x.astype(BF16)
        if not last:
            copies.append(block_copy(stage, g, out, part ^ d, width, sems))
            copies[g].start()
    contrib = dot(stage[...], w_down[...]).astype(BF16)
    atoms = sums[0].shape[0] * (shards if last else 1)
    place = lax.broadcasted_iota(jnp.int32, (atoms, width), 0)
    spread = [
        (place == relabel(targets[pl.ds(part ^ d, 1), :], me, atoms // shards)).astype(BF16)
        for d in ds
    ]
    total = dot(jnp.concatenate(spread, axis=1), contrib)
    if not first:
        total = total + acc[...]
    if last:
        share = atoms // shards
        for p in range(shards):
            sums[p][...] = total[p * share : (p + 1) * share].astype(sums[p].dtype)
    else:
        sums[0][...] = total
    for copy in copies:
        copy.wait()


def finish(ds, xs, msgs, targets, w_down, acc, out, total_rows, atoms, shards, last):
    _, width = targets.shape
    feat, hidden = w_down.shape
    first = acc is None
    assert not (first and last)
    group = len(ds)
    whole = pl.BlockSpec(memory_space=pltpu.VMEM)
    far = pl.BlockSpec(memory_space=pl.ANY)
    share = atoms // shards
    if last:
        tail = [jax.ShapeDtypeStruct((share, hidden), F32)]
        tail += [jax.ShapeDtypeStruct((share, hidden), BF16)] * (shards - 1)
    else:
        tail = [jax.ShapeDtypeStruct((atoms, hidden), F32)]
    return pl.pallas_call(
        functools.partial(finish_kernel, ds, [at for _, at in xs], first, last, shards),
        out_shape=[jax.ShapeDtypeStruct((group * width if last else total_rows, feat), BF16)] + tail,
        in_specs=[whole] * (2 * group + 2) + ([] if first else [whole] if last else [whole, far]),
        out_specs=[whole if last else far] + [whole] * len(tail),
        scratch_shapes=[]
        if last
        else [
            pltpu.VMEM((group * width, feat), BF16),
            pltpu.SemaphoreType.DMA((group,)),
        ],
        input_output_aliases={} if first or last else {2 * group + 3: 0},
        cost_estimate=pl.CostEstimate(
            flops=4 * group * width * feat * hidden,
            bytes_accessed=group * width * feat * 8,
            transcendentals=0,
        ),
        compiler_params=pltpu.CompilerParams(vmem_limit_bytes=LIMIT),
        name="finish",
    )(*[x for x, _ in xs], *msgs, targets, w_down, *([] if first else [acc] if last else [acc, out]))


def atom_kernel(atom_in, w_atom, *refs):
    *parts, out = refs
    agg = parts[0][...]
    for part in parts[1:]:
        agg = agg + part[...].astype(F32)
    v = 0.3 * agg
    act = silu(v).astype(BF16)
    out[...] = (atom_in[...].astype(F32) + dot(act, w_atom[...])).astype(BF16)


def edge_order(blocks):
    half = blocks // 2
    near = [[d, d + 1] for d in range(2, half, 2)]
    far = [[d, d + 1] for d in range(half + 2, blocks, 2)]
    return [[half, half + 1]] + near + far + [[1, 0]]


def on_device(
    edge_in, atom_in, targets, reverse, counts, w_in, gains, w_layers, w_rev, w_down, w_atom
):
    slots, feat = edge_in.shape
    blocks = counts.shape[2]
    width = slots // blocks
    shards = lax.axis_size("src")
    atoms = atom_in.shape[0] * shards
    counts = counts.reshape(1, blocks)
    targets = targets.reshape(blocks, width)
    reverse = reverse.reshape(blocks, width)

    def over(size, d):
        return [(s, s ^ d) for s in range(size)]

    held = [atom_in]
    for p in range(1, shards):
        held.append(lax.ppermute(atom_in, "src", over(shards, p)))
    weights = jnp.concatenate([w_in, w_layers.reshape(-1, feat), w_rev], axis=0)
    xs, msgs, after = {}, {}, []
    for ds in edge_order(blocks):
        x, *sent = edge_group(ds, edge_in, held, targets, reverse, counts, gains, weights, after)
        after = [x]
        for g, d in enumerate(ds):
            xs[d] = (x, g)
            msgs[d] = sent[g]
            if d:
                msgs[d] = lax.ppermute(sent[g], "dst", over(blocks, d))
    acc = out = None
    half = blocks // 2
    groups = [[0, 1, half, half + 1]]
    for rest in (list(range(2, half)), list(range(half + 2, blocks))):
        groups += [rest[n : n + 4] for n in range(0, len(rest), 4)]
    for ds in groups:
        last = ds is groups[-1]
        rows, *sums = finish(
            ds, [xs[d] for d in ds], [msgs[d] for d in ds], targets,
            w_down, acc, out, slots, atoms, shards, last,
        )
        acc = sums[0]
        if not last:
            out = rows
    parts = [sums[0]]
    for p in range(1, shards):
        parts.append(lax.ppermute(sums[p], "src", over(shards, p)))
    out = store(groups[-1], width, rows, out)
    atom_out = pl.pallas_call(
        atom_kernel,
        out_shape=jax.ShapeDtypeStruct(atom_in.shape, BF16),
        compiler_params=pltpu.CompilerParams(vmem_limit_bytes=LIMIT),
        name="atom_update",
    )(atom_in, w_atom, *parts)
    return (out, atom_out)


def solution(mesh):
    placed = (
        P(("src", "dst"), None),
        P(("dst", "src"), None),
        P(("src", "dst")),
        P(("src", "dst")),
        P("src", "dst", None),
        P(),
        P(),
        P(),
        P(),
        P(),
        P(),
    )
    return jax.shard_map(
        on_device,
        mesh=mesh,
        in_specs=placed,
        out_specs=(P(("src", "dst"), None), P(("dst", "src"), None)),
        check_vma=False,
    )
```

```python
import functools

import jax
import jax.numpy as jnp
from jax import lax
from jax.experimental import pallas as pl
from jax.experimental.pallas import tpu as pltpu
from jax.sharding import PartitionSpec as P

F32 = jnp.float32
BF16 = jnp.bfloat16
LIMIT = 16 * 2**20


def dot(a, b):
    return jnp.dot(a, b, preferred_element_type=F32)


def column(row, width):
    n = row.shape[1]
    spread = jnp.transpose(jnp.broadcast_to(row, (n, n)))
    return jnp.concatenate([spread] * (width // n), axis=1)


def relabel(row, me, share):
    return (lax.div(row, share) ^ me) * share + lax.rem(row, share)


def silu(v):
    half = 0.5 * v
    return half + half * jnp.tanh(half)


def layers(x, gains_ref, weights, first):
    feat = x.shape[1]
    for layer in range(gains_ref.shape[0]):
        scale = lax.rsqrt(jnp.mean(x * x, axis=-1, keepdims=True) + 1e-06)
        scaled = (x * gains_ref[layer : layer + 1, :]).astype(BF16)
        y = scale * dot(scaled, weights[first + layer * feat : first + (layer + 1) * feat])
        x = x + silu(y)
    return x


def edge_kernel(ds, shards, *refs):
    group = len(ds)
    me, part = lax.axis_index("src"), lax.axis_index("dst")
    edge_in, *atoms = refs[: 1 + shards]
    targets, reverse, counts, gains, weights = refs[1 + shards : 6 + shards]
    x_ref, *msgs = refs[-1 - group :]
    width = targets.shape[1]
    share = atoms[0].shape[0]
    hidden, feat = atoms[0].shape[1], edge_in.shape[1]
    w_rev = hidden + gains.shape[0] * feat
    table = jnp.concatenate([a[...] for a in atoms], axis=0)
    lanes = lax.broadcasted_iota(jnp.int32, (width, table.shape[0]), 1)
    picks = []
    for g in range(group):
        row = relabel(targets[pl.ds(part ^ ds[g], 1), :], me, share)
        picks.append((column(row, table.shape[0]) == lanes).astype(BF16))
    ready = dot(table, weights[:hidden]).astype(BF16)
    proj = dot(jnp.concatenate(picks, axis=0), ready)
    starts = [pl.multiple_of((part ^ d) * width, width) for d in ds]
    x = jnp.concatenate([edge_in[pl.ds(start, width), :] for start in starts], axis=0)
    x = x.astype(F32) + proj
    x = layers(x, gains, weights, hidden)
    sent = x.astype(BF16)
    rows = lax.broadcasted_iota(jnp.int32, (width, width), 0)
    slots = lax.broadcasted_iota(jnp.int32, (width, x.shape[1]), 0)
    turned = []
    for g in range(group):
        k = part ^ ds[g]
        lanes = lax.broadcasted_iota(jnp.int32, counts.shape, 1)
        used = jnp.sum(jnp.where(lanes == k, counts[...], 0), axis=1, keepdims=True)
        mine = slice(g * width, (g + 1) * width)
        x_ref[mine, :] = jnp.where(slots < used, x[mine], 0.0)
        swap = (rows == reverse[pl.ds(k, 1), :]) & (rows < used)
        turned.append(dot(swap.astype(BF16), sent[mine]).astype(BF16))
    msg = dot(jnp.concatenate(turned, axis=0), weights[w_rev:]).astype(BF16)
    for g in range(group):
        msgs[g][...] = msg[g * width : (g + 1) * width]


def edge_group(ds, edge_in, atoms, targets, reverse, counts, gains, weights, after):
    _, width = targets.shape
    group = len(ds)
    feat = edge_in.shape[1]
    whole = pl.BlockSpec(memory_space=pltpu.VMEM)
    rows = group * width
    return pl.pallas_call(
        functools.partial(edge_kernel, ds, len(atoms)),
        out_shape=[jax.ShapeDtypeStruct((rows, feat), F32)]
        + [jax.ShapeDtypeStruct((width, feat), BF16)] * group,
        in_specs=[whole] * (len(atoms) + 6) + [pl.BlockSpec(memory_space=pl.ANY)] * len(after),
        out_specs=[whole] * (1 + group),
        cost_estimate=pl.CostEstimate(
            flops=2 * rows * feat * feat * 4, bytes_accessed=rows * feat * 8, transcendentals=rows * feat * 4
        ),
        compiler_params=pltpu.CompilerParams(vmem_limit_bytes=LIMIT),
        name="edge_group",
    )(edge_in, *atoms, targets, reverse, counts, gains, weights, *after)


def block_copy(stage, g, out, k, width, sems):
    return pltpu.make_async_copy(
        stage.at[pl.ds(g * width, width), :],
        out.at[pl.ds(pl.multiple_of(k * width, width), width), :],
        sems.at[g],
    )


def store_kernel(ds, width, stage, old, out, sems):
    part = lax.axis_index("dst")
    copies = [block_copy(stage, g, out, part ^ d, width, sems) for g, d in enumerate(ds)]
    for copy in copies:
        copy.start()
    for copy in copies:
        copy.wait()


def store(ds, width, stage, out):
    far = pl.BlockSpec(memory_space=pl.ANY)
    return pl.pallas_call(
        functools.partial(store_kernel, ds, width),
        out_shape=jax.ShapeDtypeStruct(out.shape, out.dtype),
        in_specs=[pl.BlockSpec(memory_space=pltpu.VMEM), far],
        out_specs=far,
        scratch_shapes=[pltpu.SemaphoreType.DMA((len(ds),))],
        input_output_aliases={1: 0},
        cost_estimate=pl.CostEstimate(flops=10**8, bytes_accessed=stage.size * 4, transcendentals=0),
        compiler_params=pltpu.CompilerParams(vmem_limit_bytes=LIMIT),
        name="store",
    )(stage, out)


def finish_kernel(ds, ats, first, last, shards, *refs):
    group = len(ds)
    me, part = lax.axis_index("src"), lax.axis_index("dst")
    xs, msgs = refs[:group], refs[group : 2 * group]
    targets, w_down = refs[2 * group : 2 * group + 2]
    rest = list(refs[2 * group + 2 :])
    acc = None if first else rest[0]
    if last:
        stage, *sums = rest[1:]
    else:
        out, *sums = rest[0 if first else 2 : -2]
        stage, sems = rest[-2:]
    width = msgs[0].shape[0]
    copies = []
    for g, d in enumerate(ds):
        x = xs[g][pl.ds(ats[g] * width, width), :] + msgs[g][...].astype(F32)
        stage[pl.ds(g * width, width), :] = x.astype(BF16)
        if not last:
            copies.append(block_copy(stage, g, out, part ^ d, width, sems))
            copies[g].start()
    contrib = dot(stage[...], w_down[...]).astype(BF16)
    atoms = sums[0].shape[0] * (shards if last else 1)
    place = lax.broadcasted_iota(jnp.int32, (atoms, width), 0)
    spread = [
        (place == relabel(targets[pl.ds(part ^ d, 1), :], me, atoms // shards)).astype(BF16)
        for d in ds
    ]
    total = dot(jnp.concatenate(spread, axis=1), contrib)
    if not first:
        total = total + acc[...]
    if last:
        share = atoms // shards
        for p in range(shards):
            sums[p][...] = total[p * share : (p + 1) * share].astype(sums[p].dtype)
    else:
        sums[0][...] = total
    for copy in copies:
        copy.wait()


def finish(ds, xs, msgs, targets, w_down, acc, out, total_rows, atoms, shards, last):
    _, width = targets.shape
    feat, hidden = w_down.shape
    first = acc is None
    assert not (first and last)
    group = len(ds)
    whole = pl.BlockSpec(memory_space=pltpu.VMEM)
    far = pl.BlockSpec(memory_space=pl.ANY)
    share = atoms // shards
    if last:
        tail = [jax.ShapeDtypeStruct((share, hidden), F32)]
        tail += [jax.ShapeDtypeStruct((share, hidden), BF16)] * (shards - 1)
    else:
        tail = [jax.ShapeDtypeStruct((atoms, hidden), F32)]
    return pl.pallas_call(
        functools.partial(finish_kernel, ds, [at for _, at in xs], first, last, shards),
        out_shape=[jax.ShapeDtypeStruct((group * width if last else total_rows, feat), BF16)] + tail,
        in_specs=[whole] * (2 * group + 2) + ([] if first else [whole] if last else [whole, far]),
        out_specs=[whole if last else far] + [whole] * len(tail),
        scratch_shapes=[]
        if last
        else [
            pltpu.VMEM((group * width, feat), BF16),
            pltpu.SemaphoreType.DMA((group,)),
        ],
        input_output_aliases={} if first or last else {2 * group + 3: 0},
        cost_estimate=pl.CostEstimate(
            flops=4 * group * width * feat * hidden,
            bytes_accessed=group * width * feat * 8,
            transcendentals=0,
        ),
        compiler_params=pltpu.CompilerParams(vmem_limit_bytes=LIMIT),
        name="finish",
    )(*[x for x, _ in xs], *msgs, targets, w_down, *([] if first else [acc] if last else [acc, out]))


def atom_kernel(atom_in, w_atom, *refs):
    *parts, out = refs
    agg = parts[0][...]
    for part in parts[1:]:
        agg = agg + part[...].astype(F32)
    v = 0.3 * agg
    act = silu(v).astype(BF16)
    out[...] = (atom_in[...].astype(F32) + dot(act, w_atom[...])).astype(BF16)


def edge_order(blocks):
    half = blocks // 2
    near = [[d, d + 1] for d in range(2, half, 2)]
    far = [[d, d + 1] for d in range(half + 2, blocks, 2)]
    return [[half, half + 1]] + [near[0][:1]] + far + [near[0][1:]] + near[1:] + [[1, 0]]


def on_device(
    edge_in, atom_in, targets, reverse, counts, w_in, gains, w_layers, w_rev, w_down, w_atom
):
    slots, feat = edge_in.shape
    blocks = counts.shape[2]
    width = slots // blocks
    shards = lax.axis_size("src")
    atoms = atom_in.shape[0] * shards
    counts = counts.reshape(1, blocks)
    targets = targets.reshape(blocks, width)
    reverse = reverse.reshape(blocks, width)

    def over(size, d):
        return [(s, s ^ d) for s in range(size)]

    held = [atom_in]
    for p in range(1, shards):
        held.append(lax.ppermute(atom_in, "src", over(shards, p)))
    weights = jnp.concatenate([w_in, w_layers.reshape(-1, feat), w_rev], axis=0)
    xs, msgs, after = {}, {}, []
    for ds in edge_order(blocks):
        x, *sent = edge_group(ds, edge_in, held, targets, reverse, counts, gains, weights, after)
        after = [x]
        for g, d in enumerate(ds):
            xs[d] = (x, g)
            msgs[d] = sent[g]
            if d:
                msgs[d] = lax.ppermute(sent[g], "dst", over(blocks, d))
    acc = out = None
    half = blocks // 2
    groups = [[0, 1, half, half + 1]]
    for rest in (list(range(2, half)), list(range(half + 2, blocks))):
        groups += [rest[n : n + 4] for n in range(0, len(rest), 4)]
    for ds in groups:
        last = ds is groups[-1]
        rows, *sums = finish(
            ds, [xs[d] for d in ds], [msgs[d] for d in ds], targets,
            w_down, acc, out, slots, atoms, shards, last,
        )
        acc = sums[0]
        if not last:
            out = rows
    parts = [sums[0]]
    for p in range(1, shards):
        parts.append(lax.ppermute(sums[p], "src", over(shards, p)))
    out = store(groups[-1], width, rows, out)
    atom_out = pl.pallas_call(
        atom_kernel,
        out_shape=jax.ShapeDtypeStruct(atom_in.shape, BF16),
        compiler_params=pltpu.CompilerParams(vmem_limit_bytes=LIMIT),
        name="atom_update",
    )(atom_in, w_atom, *parts)
    return (out, atom_out)


def solution(mesh):
    placed = (
        P(("src", "dst"), None),
        P(("dst", "src"), None),
        P(("src", "dst")),
        P(("src", "dst")),
        P("src", "dst", None),
        P(),
        P(),
        P(),
        P(),
        P(),
        P(),
    )
    return jax.shard_map(
        on_device,
        mesh=mesh,
        in_specs=placed,
        out_specs=(P(("src", "dst"), None), P(("dst", "src"), None)),
        check_vma=False,
    )
```
